32 devices in a mesh: morton: 16 (over z, y, x), help: 2 (over core).
Axes of the slice: x: 2, y: 2, z: 4, core: 2. Of those that a mesh axis runs over, the one named last changes fastest.
Arguments:
- multipoles: bfloat16 [32768, 296], P(('morton', 'help')), may hold values from -6 to 6
- sources: int32 [32768, 16], P(('morton', 'help')), may hold values from 0 to 6143, as said below
- labels: int32 [32768, 16], P(('morton', 'help')), may hold values from 0 to 16, as said below
- operators: bfloat16 [16, 296, 296], replicated, may hold values from -0.375 to 0.375
Outputs:
- locals_out: float32 [32768, 296], P(('morton', 'help'))
The draws below stay inside these ranges and needn't reach their ends.
Inputs may be any that keep to these rules, and one draw needn't show every extreme that they name: The octant named by a slot, (t // (2 * 1024) - 1) * 2 * 1024 + sources[t, j], lies between 0 and 32767. `labels`: no target names one operator in two slots; the value 16 marks an empty slot.
All inputs are finite; a program needn't handle non-finite values.
Results may differ from the reference program's by a relative error of at most 0.0003.
Values may be sent and summed in bfloat16 or wider, within the bound.
No kernel may reach another device: no remote copies, remote signals or barrier semaphores. Data moves between devices by JAX's collectives and lax.ppermute only.
A program may use at most 64 MiB of HBM per device.

```python
import jax
import jax.numpy as jnp
from jax import lax

P_SIZE = 296
OPS = 16
SLOTS = 16
REACH = 1
BLOCK = 1024
OCT = 32768
N_HELP = 2


def draw_sources(key, part):
    group_rows = N_HELP * BLOCK
    groups = OCT // group_rows
    targets = jnp.arange(OCT, dtype=jnp.int32)
    group_index = targets // group_rows
    lowest = jnp.maximum(group_index - REACH, 0) * group_rows
    highest = (jnp.minimum(group_index + REACH, groups - 1) + 1) * group_rows
    named = jax.random.randint(key, (OCT, SLOTS), lowest[:, None], highest[:, None]).astype(jnp.int32)
    relative = named - ((group_index - REACH) * group_rows)[:, None]
    top_value = (2 * REACH + 1) * group_rows - 1
    relative = relative.at[REACH * group_rows, 0].set(top_value)
    return relative.astype(jnp.int32)


def draw_labels(key, part):
    first_key = jax.random.fold_in(key, 11)
    second_key = jax.random.fold_in(key, 12)
    scores = jax.random.randint(first_key, (OCT, OPS), 0, 1048576) * OPS + jnp.arange(OPS, dtype=jnp.int32)[None, :]
    ordering = jnp.argsort(scores, axis=1, stable=True).astype(jnp.int32)[:, :SLOTS]
    group_rows = N_HELP * BLOCK
    groups = OCT // group_rows
    group_index = jnp.arange(OCT, dtype=jnp.int32) // group_rows
    threshold = 300 + 650 * group_index // max(groups - 1, 1)
    rolled = jax.random.randint(second_key, (OCT, SLOTS), 0, 1000)
    return jnp.where(rolled < threshold[:, None], ordering, OPS).astype(jnp.int32)


def steps_of(key, extent, cuts, low, largest):
    loudness = 1.0
    for position, blocks in cuts:
        heights = jax.random.uniform(jax.random.fold_in(jax.random.fold_in(key, 6), position), (blocks,), jnp.float32, low / len(cuts), largest / len(cuts))
        loudness = loudness * jnp.repeat(jnp.exp(heights), extent[position] // blocks).reshape((-1,) + (1,) * (len(extent) - 1 - position))
    return loudness


def normal_values(key, dims, scale, most, shards=(), held_as=jnp.bfloat16):
    entries = scale * jax.random.normal(key, dims, jnp.float32)
    if shards:
        entries = entries * steps_of(key, dims, shards, -0.22, 0.18)
    return jnp.clip(entries, -most, most).astype(held_as)


def setup_inputs(seed: int = 0) -> dict:
    key_of = jax.random.split(jax.random.key(seed), 5)
    return {
        "multipoles": normal_values(key_of[0], (OCT, P_SIZE), 1.0, 6.0, ((0, 32),)),
        "sources": draw_sources(jax.random.fold_in(key_of[4], 71), 0),
        "labels": draw_labels(jax.random.fold_in(key_of[4], 71), 0),
        "operators": normal_values(key_of[3], (OPS, P_SIZE, P_SIZE), P_SIZE ** -0.5, 0.375),
    }


def reference(multipoles, sources, labels, operators):
    total_rows = sources.shape[0]
    block_rows = min(512, total_rows)
    block_count = total_rows // block_rows
    stacked = operators.reshape(OPS * P_SIZE, P_SIZE)
    choices_range = jnp.arange(OPS, dtype=jnp.int32)
    group_rows = N_HELP * BLOCK
    targets = jnp.arange(total_rows, dtype=jnp.int32)
    starts = ((targets // group_rows - REACH) * group_rows).astype(jnp.int32)
    named = (sources + starts[:, None]).astype(jnp.int32)

    def one_block(pieces):
        indices, kinds = pieces
        picked = jnp.take(multipoles, indices, axis=0).astype(jnp.float32)
        onehot = (kinds[:, :, None] == choices_range[None, None, :]).astype(jnp.float32)
        gathered = jnp.einsum("tjk,tjp->tkp", onehot, picked).astype(jnp.bfloat16)
        return jnp.dot(gathered.reshape(block_rows, OPS * P_SIZE), stacked, preferred_element_type=jnp.float32)

    result = lax.map(one_block, (named.reshape(block_count, block_rows, SLOTS), labels.reshape(block_count, block_rows, SLOTS)))
    return result.reshape(total_rows, P_SIZE)
```

```python
import functools

import jax
import jax.numpy as jnp
from jax import lax
from jax.experimental import pallas as pl
from jax.experimental.pallas import tpu as pltpu
from jax.sharding import PartitionSpec as P

LANES = 128
TARGETS = 256
REACH = 1


def shifted(value, axis, steps):
    count = lax.axis_size(axis)
    first, last = (max(0, -steps), min(count, count - steps))
    return lax.ppermute(value, axis, [(source, source + steps) for source in range(first, last)])


def turned(value, axis, steps):
    count = lax.axis_size(axis)
    return lax.ppermute(value, axis, [((place + steps) % count, place) for place in range(count)])


def translate_kernel(index_ref, *refs, blocks):
    block_refs = refs[:blocks]
    operator_ref, out_ref, window_ref, gathered_ref = refs[blocks:]
    features, block_rows = block_refs[0].shape
    pieces = pl.cdiv(features, LANES)
    targets = out_ref.shape[1]
    ops = index_ref.shape[0] * LANES // targets

    def lay_out(number):
        def one_tile(step, carry):
            start = pl.multiple_of(step * LANES, LANES)
            for piece in range(pieces):
                taken = min(LANES, features - piece * LANES)
                part = block_refs[number][piece * LANES:piece * LANES + taken, pl.ds(start, LANES)]
                part = part.astype(jnp.float32)
                if taken < LANES:
                    part = jnp.concatenate([part, jnp.zeros((LANES - taken, LANES), jnp.float32)], axis=0)
                first = (number * block_rows + start) * pieces + piece
                window_ref[pl.ds(first, LANES, stride=pieces), :] = part.T
            return carry

        lax.fori_loop(0, block_rows // LANES, one_tile, 0)

    for number in range(blocks):
        lay_out(number)
    window_ref[pl.ds(blocks * block_rows * pieces, 8), :] = jnp.zeros((8, LANES), jnp.float32)

    groups = TARGETS // LANES

    def one_block(block, carry):
        def one_operator(op, carry):
            for group in range(groups):
                row = index_ref.at[op * (targets // LANES) + block * groups + group]
                for lane in range(LANES):
                    slot = (op * TARGETS + group * LANES + lane) * pieces
                    gathered_ref[pl.ds(slot, pieces), :] = window_ref[pl.ds(row[lane], pieces), :]
            return carry

        lax.fori_loop(0, ops, one_operator, 0)
        left = []
        for op in range(ops):
            for piece in range(pieces):
                left.append(gathered_ref[pl.ds(op * TARGETS * pieces + piece, TARGETS, stride=pieces), :].astype(jnp.bfloat16))
        result = jnp.dot(jnp.concatenate(left, axis=1), operator_ref[...], preferred_element_type=jnp.float32)
        out_ref[:, pl.ds(pl.multiple_of(block * TARGETS, TARGETS), TARGETS)] = result.T
        return carry

    lax.fori_loop(0, targets // TARGETS, one_block, 0)


def translate(index, block_list, operators):
    ops, features, outputs = operators.shape
    targets = index.size // ops
    pieces = pl.cdiv(features, LANES)
    padded = jnp.pad(operators, ((0, 0), (0, pieces * LANES - features), (0, 0))).reshape(ops * pieces * LANES, outputs)
    in_vmem = pl.BlockSpec(memory_space=pltpu.VMEM)
    window_rows = len(block_list) * block_list[0].shape[1]
    return pl.pallas_call(
        functools.partial(translate_kernel, blocks=len(block_list)),
        out_shape=jax.ShapeDtypeStruct((outputs, targets), jnp.float32),
        in_specs=[pl.BlockSpec(memory_space=pltpu.SMEM)] + [in_vmem] * (len(block_list) + 1),
        out_specs=in_vmem,
        scratch_shapes=[
            pltpu.VMEM((window_rows * pieces + 8, LANES), jnp.float32),
            pltpu.VMEM((ops * TARGETS * pieces, LANES), jnp.float32),
        ],
        compiler_params=pltpu.CompilerParams(vmem_limit_bytes=56 * 2**20),
    )(index, *block_list, padded)


def per_device(multipoles, sources, labels, operators):
    ops, features, outputs = operators.shape
    targets = sources.shape[0]
    own = multipoles.T
    block_rows = own.shape[1]
    helpers = lax.axis_size("help")
    place = lax.axis_index("help")
    near = [shifted(own, "morton", 1), own, shifted(own, "morton", -1)]
    block_list = []
    for block in near:
        block_list.append(block)
        for step in range(1, helpers):
            block_list.append(turned(block, "help", step))

    pieces = pl.cdiv(features, LANES)
    window_rows = len(block_list) * block_rows
    rows = sources.T
    kinds = labels.T
    core = (rows // block_rows) % helpers
    rows = rows + ((core - place) % helpers - core) * block_rows
    matched = kinds[None, :, :] == jnp.arange(ops, dtype=jnp.int32)[:, None, None]
    picked = jnp.sum(jnp.where(matched, rows[None, :, :] - window_rows, 0), axis=1) + window_rows
    index = (picked * pieces).reshape(ops * targets // LANES, LANES)
    return translate(index, block_list, operators).T


def solution(mesh):
    placed = (
        P(("morton", "help"), None),
        P(("morton", "help"), None),
        P(("morton", "help"), None),
        P(),
    )
    return jax.shard_map(
        per_device,
        mesh=mesh,
        in_specs=placed,
        out_specs=P(("morton", "help"), None),
        check_vma=False,
    )
```
